32 devices in a mesh: grp: 2 (over core), dev: 16 (over z, y, x).
Axes of the slice: x: 2, y: 2, z: 4, core: 2. Of those that a mesh axis runs over, the one named last changes fastest.
Arguments:
- user_factors: float32 [4096, 256], P(('grp', 'dev')), may hold values from -0.5 to 0.5
- item_factors: float32 [2048, 256], P(('grp', 'dev')), may hold values from -0.5 to 0.5
- user_items: int32 [4096, 2, 3], P(('grp', 'dev')), may hold values from 0 to 1023, as said below
- user_conf: float32 [4096, 2, 3], P(('grp', 'dev')), may hold values from 1 to 200
- user_mask: int32 [4096, 2, 3], P(('grp', 'dev')), may hold values 0 or 1
- item_users: int32 [2048, 2, 6], P(('grp', 'dev')), may hold values from 0 to 2047, as said below
- item_conf: float32 [2048, 2, 6], P(('grp', 'dev')), may hold values from 1 to 200
- item_mask: int32 [2048, 2, 6], P(('grp', 'dev')), may hold values 0 or 1
Outputs:
- new_users: float32 [4096, 256], P(('grp', 'dev'))
- new_items: float32 [2048, 256], P(('grp', 'dev'))
The draws below stay inside these ranges and needn't reach their ends.
Inputs may be any that keep to these rules, and one draw needn't show every extreme that they name: Within owner block c, id // 64 is the owner device and id % 64 its row. The user_items of the users of one device, in one owner block, name at most 16 distinct rows of any one owner device, and in every block each device names exactly 16 distinct rows of some owner device. Within owner block c, id // 128 is the owner device and id % 128 its row. The item_users of the items of one device, in one owner block, name at most 16 distinct rows of any one owner device, and in every block each device names exactly 16 distinct rows of some owner device.
All inputs are finite; a program needn't handle non-finite values. No bound on the sum of `user_mask` or of `item_mask` on one device may be relied on, other than what follows from the above.
Results may differ from the reference program's by a relative error of at most 0.0044.
Values may be sent and summed in bfloat16 or wider, within the bound.
No kernel may reach another device: no remote copies, remote signals or barrier semaphores. Data moves between devices by JAX's collectives and lax.ppermute only.
A program may use at most 128 MiB of HBM per device.

```python
import math
import jax
import jax.numpy as jnp
from jax import lax

RANK = 256
USERS_DEV = 128
ITEMS_DEV = 64
USER_SLOTS = 3
ITEM_SLOTS = 6
REQUESTS = 16
CG_STEPS = 4
USERS = 4096
ITEMS = 2048
N_GRP = 2
N_DEV = 16


def draw_named_rows(key, total_rows, per_device, owner_rows, slots):
    keys = jax.random.split(key, 4)
    devices = total_rows // per_device
    owner = jax.random.randint(keys[0], (total_rows, N_GRP, slots), 0, N_DEV, dtype=jnp.int32)
    pick = jax.random.randint(keys[1], (total_rows, N_GRP, slots), 0, REQUESTS, dtype=jnp.int32)
    offset = jax.random.randint(keys[2], (devices, N_GRP, N_DEV), 0, owner_rows, dtype=jnp.int32)
    favored = jax.random.randint(keys[3], (devices, N_GRP), 0, N_DEV, dtype=jnp.int32)
    row_index = jnp.arange(total_rows, dtype=jnp.int32)
    device_of = (row_index // per_device).astype(jnp.int32)
    position = ((row_index % per_device)[:, None, None] * slots + jnp.arange(slots, dtype=jnp.int32)[None, None, :]).astype(jnp.int32)
    position = jnp.broadcast_to(position, (total_rows, N_GRP, slots))
    chosen = jnp.broadcast_to(favored[device_of][:, :, None], (total_rows, N_GRP, slots))
    early = position < REQUESTS
    owner = jnp.where(early, chosen, owner)
    pick = jnp.where(early, position, pick)
    block_index = jnp.broadcast_to(jnp.arange(N_GRP, dtype=jnp.int32)[None, :, None], (total_rows, N_GRP, slots))
    device_full = jnp.broadcast_to(device_of[:, None, None], (total_rows, N_GRP, slots))
    start = offset[device_full, block_index, owner]
    return (owner * owner_rows + (start + pick) % owner_rows).astype(jnp.int32)


def draw_user_items(key, part):
    return draw_named_rows(jax.random.fold_in(key, 11), USERS, USERS_DEV, ITEMS_DEV, USER_SLOTS)


def draw_item_users(key, part):
    return draw_named_rows(jax.random.fold_in(key, 23), ITEMS, ITEMS_DEV, USERS_DEV, ITEM_SLOTS)


def plant(result, key, low, largest):
    longest = result.shape.index(max(result.shape))
    spots = []
    for shift in (0, 1):
        where = [jax.random.randint(jax.random.fold_in(key, axis), (), 0, length) for axis, length in enumerate(result.shape)]
        where[longest] = (where[longest] + shift) % result.shape[longest]
        spots.append(tuple(where))
    return result.at[spots[0]].set(low).at[spots[1]].set(largest)


def block_scale(rng, dims, pieces, smallest, top_value):
    level, own = 1.0, jax.random.fold_in(rng, 6)
    for dim, parts in pieces:
        heights = jnp.exp(jax.random.uniform(jax.random.fold_in(own, dim), (parts,), jnp.float32, smallest / len(pieces), top_value / len(pieces)))
        level = level * jnp.repeat(heights, dims[dim] // parts).reshape([-1 if axis == dim else 1 for axis in range(len(dims))])
    return level


def centred(rng, shape, width, most, shards=(), kind=jnp.bfloat16):
    result = width * jax.random.normal(rng, shape, jnp.float32)
    if shards:
        result = result * block_scale(rng, shape, shards, -0.22, 0.18)
    return jnp.clip(result, -most, most).astype(kind)


def setup_inputs(seed: int = 0) -> dict:
    arg_keys = jax.random.split(jax.random.key(seed), 9)
    user_factors = centred(arg_keys[0], (USERS, RANK), 0.0625, 0.5, ((0, 32),), jnp.float32)
    item_factors = centred(arg_keys[1], (ITEMS, RANK), 0.0625, 0.5, ((0, 32),), jnp.float32)
    user_items = draw_user_items(jax.random.fold_in(arg_keys[8], 71), 0)
    user_conf = jnp.clip(jnp.exp(math.log(200.0) - 5.2983174 * jax.random.uniform(arg_keys[3], (USERS, N_GRP, USER_SLOTS), jnp.float32) ** block_scale(arg_keys[3], (USERS, N_GRP, USER_SLOTS), ((0, 32),), -0.2, 0.2)), 1.0, 200.0)
    user_mask = plant((jax.random.randint(arg_keys[4], (USERS, N_GRP, USER_SLOTS), 0, 4) < 3).astype(jnp.int32), jax.random.fold_in(arg_keys[4], 1), 0, 1)
    item_users = draw_item_users(jax.random.fold_in(arg_keys[8], 71), 0)
    item_conf = jnp.clip(jnp.exp(math.log(200.0) - 5.2983174 * jax.random.uniform(arg_keys[6], (ITEMS, N_GRP, ITEM_SLOTS), jnp.float32) ** block_scale(arg_keys[6], (ITEMS, N_GRP, ITEM_SLOTS), ((0, 32),), -0.2, 0.2)), 1.0, 200.0)
    item_mask = plant((jax.random.randint(arg_keys[7], (ITEMS, N_GRP, ITEM_SLOTS), 0, 4) < 3).astype(jnp.int32), jax.random.fold_in(arg_keys[7], 1), 0, 1)
    return {"user_factors": user_factors, "item_factors": item_factors, "user_items": user_items, "user_conf": user_conf, "user_mask": user_mask, "item_users": item_users, "item_conf": item_conf, "item_mask": item_mask}


ridge = 1.0


def solve_rows(gram, start_x, rows, confidence, slot_mask):
    maskf = slot_mask.astype(jnp.float32)
    weight = confidence * maskf
    rhs = jnp.einsum('us,usr->ur', maskf * (1.0 + confidence), rows, precision=lax.Precision.HIGHEST)

    def apply(vector):
        along = jnp.einsum('usr,ur->us', rows, vector, precision=lax.Precision.HIGHEST)
        extra = jnp.einsum('us,usr->ur', weight * along, rows, precision=lax.Precision.HIGHEST)
        return jnp.dot(vector, gram, precision=lax.Precision.HIGHEST) + ridge * vector + extra

    solution = start_x
    resid = rhs - apply(solution)
    direction = resid
    norm_now = jnp.sum(resid * resid, axis=1, keepdims=True)
    for step in range(CG_STEPS):
        image = apply(direction)
        alpha = norm_now / jnp.sum(direction * image, axis=1, keepdims=True)
        solution = solution + alpha * direction
        resid = resid - alpha * image
        norm_next = jnp.sum(resid * resid, axis=1, keepdims=True)
        direction = resid + (norm_next / norm_now) * direction
        norm_now = norm_next
    return solution


def half_step(start_x, other, slot_ids, confidence, slot_mask):
    packed = other.astype(jnp.bfloat16)
    gram = lax.dot_general(packed, packed, (((0,), (0,)), ((), ())), preferred_element_type=jnp.float32)
    block_rows = other.shape[0] // N_GRP
    total = start_x.shape[0]
    per_block = total // (N_GRP * N_DEV)
    offsets = (jnp.arange(N_GRP, dtype=jnp.int32) * block_rows).astype(jnp.int32)
    slots = slot_ids.shape[2]

    def one_block(operands):
        block_x, block_ids, block_conf, block_mask = operands
        index = (block_ids + offsets[None, :, None]).astype(jnp.int32)
        rows = packed[index].astype(jnp.float32) * block_mask[..., None].astype(jnp.float32)
        rows = rows.reshape(per_block, N_GRP * slots, -1)
        return solve_rows(gram, block_x, rows, block_conf.reshape(per_block, -1), block_mask.reshape(per_block, -1))

    shaped = (start_x.reshape(N_GRP * N_DEV, per_block, -1),
              slot_ids.reshape(N_GRP * N_DEV, per_block, N_GRP, slots),
              confidence.reshape(N_GRP * N_DEV, per_block, N_GRP, slots),
              slot_mask.reshape(N_GRP * N_DEV, per_block, N_GRP, slots))
    return lax.map(one_block, shaped).reshape(total, -1)


def reference(user_factors, item_factors, user_items, user_conf, user_mask, item_users, item_conf, item_mask):
    new_users = half_step(user_factors, item_factors, user_items, user_conf, user_mask)
    new_items = half_step(item_factors, new_users, item_users, item_conf, item_mask)
    return new_users, new_items
```

```python
import functools

import jax
import jax.numpy as jnp
from jax import lax
from jax.experimental import pallas as pl
from jax.experimental.pallas import tpu as pltpu
from jax.sharding import PartitionSpec as P

CG_STEPS = 4
RIDGE = 1.0
VMEM_LIMIT = 60 * 1024 * 1024


def swap(value, axis, bit):
    size = lax.axis_size(axis)
    return lax.ppermute(value, axis, [(i, i ^ bit) for i in range(size)])


def bits_of(size):
    return [1 << b for b in range(size.bit_length() - 1)]


def gather_pieces(own):
    rows = own.shape[0]
    low = [b for b in bits_of(lax.axis_size("dev")) if b <= 2]
    high = [b for b in bits_of(lax.axis_size("dev")) if b > 2]
    block, offsets = own, [0]
    for bit in high:
        block = jnp.concatenate([block, swap(block, "dev", bit)], axis=0)
        offsets = offsets + [o ^ bit for o in offsets]
    half = rows // 2
    shaped = block.reshape(len(offsets), rows, -1)
    parts = [
        shaped[:, :half].reshape(len(offsets) * half, -1),
        shaped[:, half:].reshape(len(offsets) * half, -1),
    ]
    marks = [list(offsets), list(offsets)]
    orders = [low, low[::-1]]
    for step in range(len(low)):
        for which in range(2):
            bit = orders[which][step]
            parts[which] = jnp.concatenate(
                [parts[which], swap(parts[which], "dev", bit)], axis=0
            )
            marks[which] = marks[which] + [o ^ bit for o in marks[which]]
    joined = jnp.concatenate(parts, axis=0)
    layout = [(0, o, 0, half) for o in marks[0]] + [(0, o, half, half) for o in marks[1]]
    pieces = [(joined, layout)]
    for bit in bits_of(lax.axis_size("grp")):
        pieces = pieces + [
            (swap(array, "grp", bit), [(g ^ bit, d, r, c) for g, d, r, c in layout])
            for array, layout in pieces
        ]
    return pieces


def split(value):
    high = value.astype(jnp.bfloat16)
    low = (value - high.astype(jnp.float32)).astype(jnp.bfloat16)
    return high, low


def dot(left, right):
    return jnp.dot(left, right, preferred_element_type=jnp.float32)


def solve_kernel(layouts, rows, devs, slots, *refs):
    count = len(layouts)
    ids_ref, start_ref, conf_ref, mask_ref = refs[:4]
    piece_refs = refs[4 : 4 + count]
    out_ref, packed_ref, table_ref, rows_ref = refs[4 + count :]
    users, rank = start_ref.shape
    me_grp, me_dev = lax.axis_index("grp"), lax.axis_index("dev")
    gram = jnp.zeros((rank, rank), jnp.float32)
    for ref, layout in zip(piece_refs, layouts):
        at = 0
        for g, d, first, length in layout:
            owner = (me_grp ^ g) * devs + (me_dev ^ d)
            where = pl.multiple_of(owner * rows + first, 8)
            table_ref[pl.ds(where, length), :] = ref[at : at + length, :].astype(jnp.float32)
            at += length
        block = ref[...]
        gram = gram + lax.dot_general(
            block, block, (((0,), (0,)), ((), ())), preferred_element_type=jnp.float32
        )

    total = rows_ref.shape[0]
    stride = total // slots * 0 + devs * rows
    per_block = slots

    def fetch(user, carry):
        for s in range(total):
            span = s // per_block
            where = ids_ref[user * total + s] + span * stride
            rows_ref[s, pl.ds(user, 1), :] = table_ref[pl.ds(where, 1), :]
        return carry

    lax.fori_loop(0, users, fetch, 0, unroll=8)

    gram_high, gram_low = split(gram)
    mask = mask_ref[...].astype(jnp.float32)
    weight = conf_ref[...] * mask
    gain = mask + weight

    def image_of(vector):
        high, low = split(vector)
        base = dot(high, gram_high) + dot(low, gram_high) + dot(high, gram_low)
        return base + RIDGE * vector

    def along(vector, s):
        return jnp.sum(rows_ref[s] * vector, axis=1, keepdims=True)

    x = start_ref[...]
    resid = -image_of(x)
    for s in range(total):
        scale = gain[:, s : s + 1] - weight[:, s : s + 1] * along(x, s)
        resid = resid + scale * rows_ref[s]
    direction = resid
    norm_now = jnp.sum(resid * resid, axis=1, keepdims=True)
    for step in range(CG_STEPS):
        image = image_of(direction)
        for s in range(total):
            image = image + (weight[:, s : s + 1] * along(direction, s)) * rows_ref[s]
        alpha = norm_now / jnp.sum(direction * image, axis=1, keepdims=True)
        x = x + alpha * direction
        if step + 1 < CG_STEPS:
            resid = resid - alpha * image
            norm_next = jnp.sum(resid * resid, axis=1, keepdims=True)
            direction = resid + (norm_next / norm_now) * direction
            norm_now = norm_next
    out_ref[...] = x
    packed_ref[...] = x.astype(jnp.bfloat16)


def half_step(start_x, packed, slot_ids, confidence, slot_mask):
    users, rank = start_x.shape
    rows = packed.shape[0]
    groups, devs = lax.axis_size("grp"), lax.axis_size("dev")
    slots = slot_ids.shape[2]
    total = groups * slots
    pieces = gather_pieces(packed)
    vmem = pl.BlockSpec(memory_space=pltpu.VMEM)
    return pl.pallas_call(
        functools.partial(solve_kernel, [p[1] for p in pieces], rows, devs, slots),
        out_shape=(
            jax.ShapeDtypeStruct((users, rank), jnp.float32),
            jax.ShapeDtypeStruct((users, rank), jnp.bfloat16),
        ),
        in_specs=[pl.BlockSpec(memory_space=pltpu.SMEM)] + [vmem] * (3 + len(pieces)),
        out_specs=(vmem, vmem),
        scratch_shapes=[
            pltpu.VMEM((groups * devs * rows, rank), jnp.float32),
            pltpu.VMEM((total, users, rank), jnp.float32),
        ],
        compiler_params=pltpu.CompilerParams(vmem_limit_bytes=VMEM_LIMIT),
    )(
        slot_ids.reshape(-1),
        start_x,
        confidence.reshape(users, total),
        slot_mask.reshape(users, total),
        *[p[0] for p in pieces],
    )


def per_device(
    user_factors, item_factors, user_items, user_conf, user_mask, item_users, item_conf, item_mask
):
    new_users, packed = half_step(
        user_factors, item_factors.astype(jnp.bfloat16), user_items, user_conf, user_mask
    )
    new_items, _ = half_step(item_factors, packed, item_users, item_conf, item_mask)
    return (new_users, new_items)


def solution(mesh):
    rows2 = P(("grp", "dev"), None)
    rows3 = P(("grp", "dev"), None, None)
    return jax.shard_map(
        per_device,
        mesh=mesh,
        in_specs=(rows2, rows2) + (rows3,) * 6,
        out_specs=(rows2, rows2),
        check_vma=False,
    )
```

```python
import functools

import jax
import jax.numpy as jnp
from jax import lax
from jax.experimental import pallas as pl
from jax.experimental.pallas import tpu as pltpu
from jax.sharding import PartitionSpec as P

CG_STEPS = 4
RIDGE = 1.0
LANES = 128
MIB = 1024 * 1024


def swap(value, axis, bit):
    size = lax.axis_size(axis)
    return lax.ppermute(value, axis, [(i, i ^ bit) for i in range(size)])


def bits_of(size):
    return [1 << b for b in range(size.bit_length() - 1)]


def gather_pieces(own, axis):
    bits = bits_of(lax.axis_size("dev"))
    low = [b for b in bits if b <= 2]
    high = [b for b in bits if b > 2]
    block, marks = own, [0]
    for bit in high[::-1]:
        block = jnp.concatenate([block, swap(block, "dev", bit)], axis=axis)
        marks = marks + [o ^ bit for o in marks]
    pieces = [(block, marks)]
    if len(marks) > 1:
        half = len(marks) // 2
        pieces = list(zip(jnp.split(block, 2, axis=axis), (marks[:half], marks[half:])))
    orders = [low, low[::-1]]
    for step in range(len(low)):
        for which, (block, marks) in enumerate(pieces):
            bit = orders[which][step]
            block = jnp.concatenate([block, swap(block, "dev", bit)], axis=axis)
            pieces[which] = (block, marks + [o ^ bit for o in marks])
    pieces = [(block, [(0, o) for o in marks]) for block, marks in pieces]
    for bit in bits_of(lax.axis_size("grp")):
        pieces = pieces + [
            (swap(block, "grp", bit), [(g ^ bit, o) for g, o in marks]) for block, marks in pieces
        ]
    return pieces


def split(value):
    high = value.astype(jnp.bfloat16)
    low = (value - high.astype(jnp.float32)).astype(jnp.bfloat16)
    return high, low


def solve_kernel(marks, axis, rows, groups, *refs):
    count = len(marks)
    start_ref, ids_ref, conf_ref, mask_ref = refs[:4]
    piece_refs = refs[4 : 4 + count]
    out_ref, packed_ref, hot_ref, rows_ref, gram_ref = refs[4 + count :]
    users, rank = start_ref.shape
    slots = ids_ref.shape[0]
    pack = max(1, LANES // users)
    width = pack * users
    tiles = slots // pack
    me_grp, me_dev = lax.axis_index("grp"), lax.axis_index("dev")

    def row_of(ref, g, tile):
        block = me_grp ^ g
        parts = [ref[tile * pack + i, pl.ds(block, 1), :] for i in range(pack)]
        return parts[0] if pack == 1 else jnp.concatenate(parts, axis=1)

    weights, gains = [], []
    for g in range(groups):
        for tile in range(tiles):
            mask = row_of(mask_ref, g, tile).astype(jnp.float32)
            weight = row_of(conf_ref, g, tile) * mask
            weights.append(weight)
            gains.append(mask + weight)

    side = (((axis,), (axis,)), ((), ()))
    gram = jnp.zeros((rank, rank), jnp.float32)
    place = lax.broadcasted_iota(jnp.int32, (rows, width), 0)
    seen = set()
    for ref, mark in zip(piece_refs, marks):
        g = mark[0][0]
        for tile in range(tiles):
            ids = row_of(ids_ref, g, tile)
            for j, (_, d) in enumerate(mark):
                local = ids - (me_dev ^ d) * rows
                hot_ref[j * rows : (j + 1) * rows, tile * width : (tile + 1) * width] = jnp.where(
                    place == local, 1.0, 0.0
                ).astype(jnp.bfloat16)
        block = ref[...]
        gram = gram + lax.dot_general(block, block, side, preferred_element_type=jnp.float32)
        hot = hot_ref[: len(mark) * rows, :]
        found = lax.dot_general(
            block, hot, (((axis,), (0,)), ((), ())), preferred_element_type=jnp.float32
        )
        for tile in range(tiles):
            part = found[:, tile * width : (tile + 1) * width]
            at = g * tiles + tile
            rows_ref[at] = rows_ref[at] + part if g in seen else part
        seen.add(g)
    high, low = split(gram)
    gram_ref[:rank, :] = high
    gram_ref[rank:, :] = low

    def fold(value):
        if pack == 1:
            return value
        return value + pltpu.roll(value, users, 1)

    def image_of(vector):
        both = jnp.concatenate(split(vector), axis=1)
        image = jnp.dot(gram_ref[...], both, preferred_element_type=jnp.float32)
        image = image[:rank] + image[rank:]
        return image[:, :width] + image[:, width:] + RIDGE * vector

    def along(vector, at):
        return jnp.sum(rows_ref[at] * vector, axis=0, keepdims=True)

    x = start_ref[...].T
    if pack > 1:
        x = jnp.concatenate([x] * pack, axis=1)
    extra = jnp.zeros_like(x)
    for at in range(groups * tiles):
        extra = extra + (gains[at] - weights[at] * along(x, at)) * rows_ref[at]
    resid = fold(extra) - image_of(x)
    direction = resid
    norm_now = jnp.sum(resid * resid, axis=0, keepdims=True)
    for step in range(CG_STEPS):
        extra = jnp.zeros_like(x)
        for at in range(groups * tiles):
            extra = extra + (weights[at] * along(direction, at)) * rows_ref[at]
        image = fold(extra) + image_of(direction)
        alpha = norm_now / jnp.sum(direction * image, axis=0, keepdims=True)
        x = x + alpha * direction
        if step + 1 < CG_STEPS:
            resid = resid - alpha * image
            norm_next = jnp.sum(resid * resid, axis=0, keepdims=True)
            direction = resid + (norm_next / norm_now) * direction
            norm_now = norm_next
    x = x[:, :users]
    packed_ref[...] = x.astype(jnp.bfloat16)
    out_ref[...] = x.T


def half_step(start_x, own, axis, slot_ids, confidence, slot_mask):
    users, rank = start_x.shape
    rows = own.shape[axis]
    groups = slot_ids.shape[1]
    pieces = gather_pieces(own, axis)
    most = max(len(m) for _, m in pieces) * rows
    lanes = slot_ids.shape[2] * users
    vmem = pl.BlockSpec(memory_space=pltpu.VMEM)
    table = sum(p.size for p, _ in pieces) * 2
    return pl.pallas_call(
        functools.partial(solve_kernel, [m for _, m in pieces], axis, rows, groups),
        out_shape=(
            jax.ShapeDtypeStruct((users, rank), jnp.float32),
            jax.ShapeDtypeStruct((rank, users), jnp.bfloat16),
        ),
        in_specs=[vmem] * (4 + len(pieces)),
        out_specs=(vmem, vmem),
        scratch_shapes=[
            pltpu.VMEM((most, lanes), jnp.bfloat16),
            pltpu.VMEM((groups * lanes // max(users, LANES), rank, max(users, LANES)), jnp.float32),
            pltpu.VMEM((2 * rank, rank), jnp.bfloat16),
        ],
        compiler_params=pltpu.CompilerParams(
            vmem_limit_bytes=(16 if table <= 4 * MIB else 60) * MIB
        ),
    )(
        start_x,
        slot_ids.transpose(2, 1, 0),
        confidence.transpose(2, 1, 0),
        slot_mask.transpose(2, 1, 0),
        *[p for p, _ in pieces],
    )


def per_device(
    user_factors, item_factors, user_items, user_conf, user_mask, item_users, item_conf, item_mask
):
    packed = item_factors.astype(jnp.bfloat16)
    new_users, packed = half_step(user_factors, packed, 0, user_items, user_conf, user_mask)
    new_items, _ = half_step(item_factors, packed, 1, item_users, item_conf, item_mask)
    return (new_users, new_items)


def solution(mesh):
    rows2 = P(("grp", "dev"), None)
    rows3 = P(("grp", "dev"), None, None)
    return jax.shard_map(
        per_device,
        mesh=mesh,
        in_specs=(rows2, rows2) + (rows3,) * 6,
        out_specs=(rows2, rows2),
        check_vma=False,
    )
```

```python
import functools

import jax
import jax.numpy as jnp
from jax import lax
from jax.experimental import pallas as pl
from jax.experimental.pallas import tpu as pltpu
from jax.sharding import PartitionSpec as P


CG_STEPS = 4
RIDGE = 1.0
LANES = 128
SHORT = 48 * 1024
MIB = 1024 * 1024


def swap(value, axis, bit):
    size = lax.axis_size(axis)
    return lax.ppermute(value, axis, [(i, i ^ bit) for i in range(size)])


def bits_of(size):
    return [1 << b for b in range(size.bit_length() - 1)]


def gather_pieces(own, axis):
    first, second, near, *far = bits_of(lax.axis_size("dev"))

    def move(piece, bit):
        block, marks = piece
        return swap(block, "dev", bit), [o ^ bit for o in marks]

    def join(pieces):
        return jnp.concatenate([b for b, _ in pieces], axis=axis), sum((m for _, m in pieces), [])

    def mine(piece):
        return piece[0], [(0, o) for o in piece[1]]

    def spread(piece):
        group = [mine(piece)]
        for bit in bits_of(lax.axis_size("grp")):
            group = group + [(swap(b, "grp", bit), [(g ^ bit, o) for g, o in m]) for b, m in group]
        return group

    a = (own, [0])
    if own.size * 2 <= SHORT:
        for bit in far[::-1]:
            a = join([a, move(a, bit)])
        b = move(a, near)
        ax, ay = move(a, first), move(a, second)
        bx = move(b, first)
        more = move(join([ax, b]), second)
        last = move(bx, second)
        one = spread(join([a, b, ax, ay, bx]))
        two = spread(join([more, last]))
        return one, [mine(more)], [mine(last)], two[1:]
    b = None
    for bit in far[::-1]:
        moved = move(a, bit)
        if b is None:
            b = move(a, near)
        b = join([b, move(moved, near)])
        a = join([a, moved])
    ax, ay = move(a, first), move(a, second)
    bx, by = move(b, first), move(b, second)
    axy = move(ay, first)
    bxy = move(bx, second)
    one = spread(join([a, b, ax, ay]))
    two = spread(join([bx, by, axy]))
    three = spread(bxy)
    return one, two, three[:1], three[1:]


def split(value):
    high = value.astype(jnp.bfloat16)
    low = (value - high.astype(jnp.float32)).astype(jnp.bfloat16)
    return high, low


def shape_of(ids_ref, users):
    pack = max(1, LANES // users)
    return pack, pack * users, ids_ref.shape[0] // pack


def row_of(ref, g, tile, pack):
    block = lax.axis_index("grp") ^ g
    parts = [ref[tile * pack + i, pl.ds(block, 1), :] for i in range(pack)]
    return parts[0] if pack == 1 else jnp.concatenate(parts, axis=1)


def absorb(marks, axis, rows, users, ids_ref, piece_refs, hot_ref, gram, table_ref, seen):
    pack, width, tiles = shape_of(ids_ref, users)
    me_dev = lax.axis_index("dev")
    side = (((axis,), (axis,)), ((), ()))
    place = lax.broadcasted_iota(jnp.int32, (rows, width), 0)
    for ref, mark in zip(piece_refs, marks):
        g = mark[0][0]
        for tile in range(tiles):
            ids = row_of(ids_ref, g, tile, pack)
            for j, (_, d) in enumerate(mark):
                local = ids - (me_dev ^ d) * rows
                hot_ref[j * rows : (j + 1) * rows, tile * width : (tile + 1) * width] = jnp.where(
                    place == local, 1.0, 0.0
                ).astype(jnp.bfloat16)
        block = ref[...]
        part = lax.dot_general(block, block, side, preferred_element_type=jnp.float32)
        gram = part if gram is None else gram + part
        hot = hot_ref[: len(mark) * rows, :]
        found = lax.dot_general(
            block, hot, (((axis,), (0,)), ((), ())), preferred_element_type=jnp.float32
        )
        for tile in range(tiles):
            part = found[:, tile * width : (tile + 1) * width]
            at = g * tiles + tile
            table_ref[at] = table_ref[at] + part if g in seen else part
        seen.add(g)
    return gram


def early_kernel(marks, axis, rows, *refs, groups):
    count = len(marks)
    ids_ref, conf_ref, mask_ref, start_ref = refs[:4]
    piece_refs = refs[4 : 4 + count]
    gram_out, table_out, x_out, weight_out, gain_out, hot_ref = refs[4 + count :]
    users = start_ref.shape[0]
    pack, _, tiles = shape_of(ids_ref, users)
    for g in range(groups):
        for tile in range(tiles):
            at = g * tiles + tile
            mask = row_of(mask_ref, g, tile, pack).astype(jnp.float32)
            weight = row_of(conf_ref, g, tile, pack) * mask
            weight_out[at : at + 1, :] = weight
            gain_out[at : at + 1, :] = mask + weight
    x = start_ref[...].T
    x_out[...] = x if pack == 1 else jnp.concatenate([x] * pack, axis=1)
    gram_out[...] = absorb(
        marks, axis, rows, users, ids_ref, piece_refs, hot_ref, None, table_out, set()
    )


def own_kernel(marks, axis, rows, *refs, users):
    count = len(marks)
    ids_ref, gram_in, table_in = refs[:3]
    piece_refs = refs[3 : 3 + count]
    gram_out, table_out, hot_ref = refs[3 + count :]
    for at in range(table_in.shape[0]):
        table_out[at] = table_in[at]
    gram_out[...] = absorb(
        marks, axis, rows, users, ids_ref, piece_refs, hot_ref, gram_in[...], table_out,
        {m[0][0] for m in marks},
    )


def solve_kernel(marks, axis, rows, *refs, groups, users):
    count = len(marks)
    ids_ref, gram_in, table_ref, start_ref, weight_ref, gain_ref = refs[:6]
    piece_refs = refs[6 : 6 + count]
    out_ref, packed_ref, rows_ref, hot_ref, gram_ref = refs[6 + count :]
    rank = start_ref.shape[0]
    pack, width, tiles = shape_of(ids_ref, users)
    weights = [weight_ref[at : at + 1, :] for at in range(groups * tiles)]
    gains = [gain_ref[at : at + 1, :] for at in range(groups * tiles)]

    touched = {m[0][0] for m in marks}
    for at in range(groups * tiles):
        rows_ref[at] = table_ref[at]
    gram = absorb(
        marks, axis, rows, users, ids_ref, piece_refs, hot_ref, gram_in[...], rows_ref, touched
    )
    high, low = split(gram)
    gram_ref[:rank, :] = high
    gram_ref[rank:, :] = low

    def fold(value):
        if pack == 1:
            return value
        return value + pltpu.roll(value, users, 1)

    def image_of(vector):
        both = jnp.concatenate(split(vector), axis=1)
        image = jnp.dot(gram_ref[...], both, preferred_element_type=jnp.float32)
        image = image[:rank] + image[rank:]
        return image[:, :width] + image[:, width:] + RIDGE * vector

    def along(vector, at):
        return jnp.sum(rows_ref[at] * vector, axis=0, keepdims=True)

    x = start_ref[...]
    extra = jnp.zeros_like(x)
    for at in range(groups * tiles):
        extra = extra + (gains[at] - weights[at] * along(x, at)) * rows_ref[at]
    resid = fold(extra) - image_of(x)
    direction = resid
    norm_now = jnp.sum(resid * resid, axis=0, keepdims=True)
    for step in range(CG_STEPS):
        extra = jnp.zeros_like(x)
        for at in range(groups * tiles):
            extra = extra + (weights[at] * along(direction, at)) * rows_ref[at]
        image = fold(extra) + image_of(direction)
        alpha = norm_now / jnp.sum(direction * image, axis=0, keepdims=True)
        x = x + alpha * direction
        if step + 1 < CG_STEPS:
            resid = resid - alpha * image
            norm_next = jnp.sum(resid * resid, axis=0, keepdims=True)
            direction = resid + (norm_next / norm_now) * direction
            norm_now = norm_next
    x = x[:, :users]
    packed_ref[...] = x.astype(jnp.bfloat16)
    out_ref[...] = x if out_ref.shape == x.shape else x.T


def half_step(start_x, own, axis, slot_ids, confidence, slot_mask):
    users, rank = start_x.shape
    rows = own.shape[axis]
    groups, slots = slot_ids.shape[1:]
    first, second, third, fourth = gather_pieces(own, axis)
    ids = slot_ids.transpose(2, 1, 0)
    width = max(users, LANES)
    lanes = slots * users
    vmem = pl.BlockSpec(memory_space=pltpu.VMEM)
    small = lax.axis_size("dev") * groups * rows * rank <= 2 * MIB
    params = pltpu.CompilerParams(vmem_limit_bytes=(16 if small else 60) * MIB)
    gram_shape = jax.ShapeDtypeStruct((rank, rank), jnp.float32)
    table_shape = jax.ShapeDtypeStruct((groups * lanes // width, rank, width), jnp.float32)

    def hot_scratch(pieces):
        return pltpu.VMEM((max(len(m) for _, m in pieces) * rows, lanes), jnp.bfloat16)

    def cost(pieces):
        table = sum(p.size for p, _ in pieces)
        return pl.CostEstimate(
            flops=2 * table * (rank + lanes), bytes_accessed=2 * table, transcendentals=0
        )

    def call(kernel, pieces, operands, out_shape, scratch):
        return pl.pallas_call(
            functools.partial(kernel, [m for _, m in pieces], axis, rows),
            out_shape=out_shape,
            in_specs=[vmem] * (len(operands) + len(pieces)),
            out_specs=(vmem,) * len(out_shape),
            scratch_shapes=scratch,
            compiler_params=params,
            cost_estimate=cost(pieces),
        )(*operands, *[p for p, _ in pieces])

    tiles = table_shape.shape[0]
    line_shape = jax.ShapeDtypeStruct((tiles, width), jnp.float32)
    gram, table, start, weight, gain = call(
        functools.partial(early_kernel, groups=groups),
        first,
        (ids, confidence.transpose(2, 1, 0), slot_mask.transpose(2, 1, 0), start_x),
        (gram_shape, table_shape, jax.ShapeDtypeStruct((rank, width), jnp.float32), line_shape, line_shape),
        [hot_scratch(first)],
    )
    for pieces in (second, third):
        gram, table = call(
            functools.partial(own_kernel, users=users),
            pieces,
            (ids, gram, table),
            (gram_shape, table_shape),
            [hot_scratch(pieces)],
        )
    return call(
        functools.partial(solve_kernel, groups=groups, users=users),
        fourth,
        (ids, gram, table, start, weight, gain),
        (
            jax.ShapeDtypeStruct((rank, users) if axis == 0 else (users, rank), jnp.float32),
            jax.ShapeDtypeStruct((rank, users), jnp.bfloat16),
        ),
        [
            pltpu.VMEM(table_shape.shape, jnp.float32),
            hot_scratch(fourth),
            pltpu.VMEM((2 * rank, rank), jnp.bfloat16),
        ],
    )


def turn_kernel(value_ref, out_ref):
    out_ref[...] = value_ref[...].T


def turn(value):
    vmem = pl.BlockSpec(memory_space=pltpu.VMEM)
    return pl.pallas_call(
        turn_kernel,
        out_shape=jax.ShapeDtypeStruct(value.shape[::-1], value.dtype),
        in_specs=[vmem],
        out_specs=vmem,
        compiler_params=pltpu.CompilerParams(vmem_limit_bytes=8 * MIB),
        name="turn",
    )(value)


def per_device(
    user_factors, item_factors, user_items, user_conf, user_mask, item_users, item_conf, item_mask
):
    packed = item_factors.astype(jnp.bfloat16)
    new_users, packed = half_step(user_factors, packed, 0, user_items, user_conf, user_mask)
    new_users = turn(new_users)
    new_items, _ = half_step(item_factors, packed, 1, item_users, item_conf, item_mask)
    return (new_users, new_items)


def solution(mesh):
    rows2 = P(("grp", "dev"), None)
    rows3 = P(("grp", "dev"), None, None)
    return jax.shard_map(
        per_device,
        mesh=mesh,
        in_specs=(rows2, rows2) + (rows3,) * 6,
        out_specs=(rows2, rows2),
        check_vma=False,
    )
```
